512 devices in a mesh: section: 2 (over y_lo), grp: 32 (over z, core), tp: 8 (over x, y_hi).
Axes of the slice: x: 4, y: 4 (y_hi: 2, y_lo: 2; y = y_hi * 2 + y_lo), z: 16, core: 2. Of those that a mesh axis runs over, the one named last changes fastest.
Arguments:
- partials: bfloat16 [8, 2, 4096, 8192], P('tp', 'section', 'grp'), may hold values from -3 to 3
- residual: bfloat16 [2, 4096, 8192], P('section', 'grp', 'tp'), may hold values from -300 to 300
- norm_gain: bfloat16 [8192], replicated, may hold values from 0.099609375 to 1.8984375
- w_query: bfloat16 [8192, 8192], P('grp', ('section', 'tp')), may hold values from -0.0625 to 0.0625
- w_keyval: bfloat16 [8192, 2048], P('grp', ('section', 'tp')), may hold values from -0.0625 to 0.0625
- bias_query: bfloat16 [8192], P(('section', 'tp')), may hold values from -3 to 3
- bias_keyval: bfloat16 [2048], P(('section', 'tp')), may hold values from -3 to 3
Outputs:
- hidden: bfloat16 [2, 4096, 8192], P('section', 'grp', 'tp')
- query: bfloat16 [2, 4096, 8192], P(None, 'grp', ('section', 'tp'))
- keyval: bfloat16 [2, 4096, 2048], P(None, 'grp', ('section', 'tp'))
The draws below stay inside these ranges and needn't reach their ends.
All inputs are finite; a program needn't handle non-finite values.
Results may differ from the reference program's by a relative error of at most 0.01.
Values may be sent and summed in bfloat16 or wider, within the bound.
No kernel may reach another device: no remote copies, remote signals or barrier semaphores. Data moves between devices by JAX's collectives and lax.ppermute only.
A program may use at most 64 MiB of HBM per device.

```python
import jax
import jax.numpy as jnp
from jax import lax

D = 8192
LEN = 4096
SEQS = 2
PARTS_SIZE = 8
QCOLS = 8192
KVCOLS = 2048


def draw_residual(key, part):
    base_key = jax.random.fold_in(key, 11)
    key_normal, key_jitter, key_rows = jax.random.split(base_key, 3)
    column_ramp = 10.0 ** (jnp.arange(D, dtype=jnp.float32) / D)
    column_jitter = jax.random.uniform(key_jitter, (D,), jnp.float32, 0.5, 1.5)
    normal_part = jnp.clip(jax.random.normal(key_normal, (SEQS, LEN, D), jnp.float32), -4.0, 4.0)
    row_scale = 10.0 ** jax.random.uniform(key_rows, (SEQS, LEN, 1), jnp.float32, 0.0, 1.0)
    values = 0.3 * normal_part * column_ramp * column_jitter * row_scale
    return values.astype(jnp.bfloat16)


def block_levels(key, dims, cuts, low, high):
    factor_of = 1.0
    for axis_at, parts in cuts:
        draws = jax.random.uniform(jax.random.fold_in(jax.random.fold_in(key, 6), axis_at), (parts,), jnp.float32, low / len(cuts), high / len(cuts))
        factor_of = factor_of * jnp.repeat(jnp.exp(draws), dims[axis_at] // parts).reshape((-1,) + (1,) * (len(dims) - 1 - axis_at))
    return factor_of


def bell_draw(key, dims, deviation, limit, shards=(), kind=jnp.bfloat16):
    entries = jax.random.normal(key, dims, jnp.float32) * deviation
    if len(shards) > 0:
        entries = block_levels(key, dims, shards, -0.22, 0.18) * entries
    return jnp.clip(entries, min=-limit, max=limit).astype(kind)


def setup_inputs(seed: int = 0) -> dict:
    keys = jax.random.split(jax.random.key(seed), 8)
    partials = bell_draw(keys[0], (PARTS_SIZE, SEQS, LEN, D), 0.5, 3.0, ((0, 8), (1, 2), (2, 32)))
    residual = draw_residual(jax.random.fold_in(keys[7], 71), 0)
    norm_gain = jnp.clip(1.0 + 0.18 * jax.random.normal(keys[2], (D,), jnp.float32), 0.099609375, 1.8984375).astype(jnp.bfloat16)
    w_query = bell_draw(keys[3], (D, QCOLS), D ** -0.5, 0.0625, ((0, 32), (1, 16)))
    w_keyval = bell_draw(keys[4], (D, KVCOLS), D ** -0.5, 0.0625, ((0, 32), (1, 16)))
    bias_query = bell_draw(keys[5], (QCOLS,), 0.5, 3.0, ((0, 16),))
    bias_keyval = bell_draw(keys[6], (KVCOLS,), 0.5, 3.0, ((0, 16),))
    return {"partials": partials, "residual": residual, "norm_gain": norm_gain, "w_query": w_query, "w_keyval": w_keyval, "bias_query": bias_query, "bias_keyval": bias_keyval}


epsilon = 1e-06

def reference(partials, residual, norm_gain, w_query, w_keyval, bias_query, bias_keyval):
    summed = jnp.zeros(residual.shape, jnp.float32)
    for part_index in range(PARTS_SIZE):
        summed = summed + partials[part_index].astype(jnp.float32)
    hidden = (residual.astype(jnp.float32) + summed).astype(jnp.bfloat16)
    widened = hidden.astype(jnp.float32)
    mean_square = lax.optimization_barrier(jnp.mean(widened * widened, axis=-1, keepdims=True))
    normed = (widened * lax.rsqrt(mean_square + epsilon) * norm_gain.astype(jnp.float32)).astype(jnp.bfloat16)
    flattened = normed.reshape(SEQS * LEN, D)
    query = jnp.dot(flattened, w_query, preferred_element_type=jnp.float32) + bias_query.astype(jnp.float32)
    keyval = jnp.dot(flattened, w_keyval, preferred_element_type=jnp.float32) + bias_keyval.astype(jnp.float32)
    query = query.astype(jnp.bfloat16).reshape(SEQS, LEN, QCOLS)
    keyval = keyval.astype(jnp.bfloat16).reshape(SEQS, LEN, KVCOLS)
    return (hidden, query, keyval)
```

```python
import jax
import jax.numpy as jnp
from jax import lax
from jax.experimental import pallas as pl
from jax.experimental.pallas import tpu as pltpu
from jax.sharding import PartitionSpec as P

epsilon = 1e-06
MESH_AXES = ("section", "grp", "tp")


def plane_groups(mesh, along_x_core):
    n_sec, n_grp, n_tp = (mesh.shape[a] for a in MESH_AXES)

    def device(x, y, g):
        y_hi, y_lo = divmod(y, n_sec)
        return (y_lo * n_grp + g) * n_tp + x * 2 + y_hi

    n_x, n_y = n_tp // 2, 2 * n_sec
    groups = []
    for g in range(n_grp):
        if g % 2 == along_x_core:
            groups += [[device(x, y, g) for x in range(n_x)] for y in range(n_y)]
        else:
            groups += [[device(x, y, g) for y in range(n_y)] for x in range(n_x)]
    return groups


def copy_body(src, dst):
    dst[0] = src[...]


def blocks_of_features(partial, blocks):
    rows, width = partial.shape
    share = width // blocks
    return pl.pallas_call(
        copy_body,
        grid=(blocks,),
        in_specs=[pl.BlockSpec((rows, share), lambda i: (0, i))],
        out_specs=pl.BlockSpec((1, rows, share), lambda i: (i, 0, 0)),
        out_shape=jax.ShapeDtypeStruct((blocks, rows, share), partial.dtype),
        name="cut_features",
    )(partial)


def project_body(table, first, second, gain, weights, bias, query, keyval, total, squares):
    step = pl.program_id(0)
    rows = first.shape[1]

    @pl.when(step == 0)
    def _():
        total[...] = jnp.zeros_like(total)
        squares[...] = jnp.zeros_like(squares)

    scale = gain[0].astype(jnp.float32)
    for s, block in enumerate((first, second)):
        at = pl.ds(s * rows, rows)
        hidden = block[0].astype(jnp.float32)
        squares[at, :] += jnp.sum(hidden * hidden, axis=-1, keepdims=True)
        scaled = (hidden * scale).astype(jnp.bfloat16)
        total[at, :] += jnp.dot(scaled, weights[...], preferred_element_type=jnp.float32)

    @pl.when(step == pl.num_programs(0) - 1)
    def _():
        width = pl.num_programs(0) * first.shape[2]
        root = lax.rsqrt(squares[...] / width + epsilon)
        result = total[...] * root + bias[...].astype(jnp.float32)
        split = query.shape[2]
        for s in range(2):
            at = slice(s * rows, (s + 1) * rows)
            query[s] = result[at, :split].astype(query.dtype)
            keyval[s] = result[at, split:].astype(keyval.dtype)


def project(table, gathered, gain, weights, bias, query_width):
    _, rows, share = gathered.shape
    width, cols = weights.shape
    steps = width // share
    block = (1, rows, share)
    return pl.pallas_call(
        project_body,
        grid_spec=pltpu.PrefetchScalarGridSpec(
            num_scalar_prefetch=1,
            grid=(steps,),
            in_specs=[
                pl.BlockSpec(block, lambda k, t: (t[0, k], 0, 0)),
                pl.BlockSpec(block, lambda k, t: (t[1, k], 0, 0)),
                pl.BlockSpec((1, 1, share), lambda k, t: (k, 0, 0)),
                pl.BlockSpec((share, cols), lambda k, t: (k, 0)),
                pl.BlockSpec((1, cols), lambda k, t: (0, 0)),
            ],
            out_specs=[
                pl.BlockSpec((2, rows, query_width), lambda k, t: (0, 0, 0)),
                pl.BlockSpec((2, rows, cols - query_width), lambda k, t: (0, 0, 0)),
            ],
            scratch_shapes=[
                pltpu.VMEM((2 * rows, cols), jnp.float32),
                pltpu.VMEM((2 * rows, 1), jnp.float32),
            ],
        ),
        out_shape=[
            jax.ShapeDtypeStruct((2, rows, query_width), jnp.bfloat16),
            jax.ShapeDtypeStruct((2, rows, cols - query_width), jnp.bfloat16),
        ],
        name="project",
    )(table, gathered, gathered, gain.reshape(steps, 1, share), weights, bias)


def spread(value, groups):
    copies = jnp.broadcast_to(value, (4, *value.shape))
    return lax.all_to_all(copies, MESH_AXES, split_axis=0, concat_axis=0, tiled=True, axis_index_groups=groups)


def solution(mesh):
    first_groups = plane_groups(mesh, 1)
    second_groups = plane_groups(mesh, 0)

    def local(partials, residual, norm_gain, w_query, w_keyval, bias_query, bias_keyval):
        weights = lax.all_gather(jnp.concatenate([w_query, w_keyval], axis=1), "grp", axis=0, tiled=True)
        n_tp = lax.axis_size("tp")
        parts = blocks_of_features(partials[0, 0], n_tp)
        arrived = lax.all_to_all(parts, "tp", split_axis=0, concat_axis=0, tiled=True)
        summed = arrived.astype(jnp.float32).sum(axis=0)
        hidden = (residual[0].astype(jnp.float32) + summed).astype(jnp.bfloat16)
        gathered = spread(spread(hidden, first_groups), second_groups)
        gathered = gathered.reshape(16, *hidden.shape)
        core = lax.axis_index("grp") % 2
        section = jnp.arange(2)[:, None]
        part = jnp.arange(n_tp)[None, :]
        along_y = part * 2 + section
        along_x = (part % 2) * 8 + section * 4 + part // 2
        table = jnp.where(core == 0, along_y, along_x).astype(jnp.int32)
        bias = jnp.concatenate([bias_query, bias_keyval])[None, :]
        query, keyval = project(table, gathered, norm_gain, weights, bias, w_query.shape[1])
        return hidden[None], query, keyval

    placed = (
        P("tp", "section", "grp", None),
        P("section", "grp", "tp"),
        P(),
        P("grp", ("section", "tp")),
        P("grp", ("section", "tp")),
        P(("section", "tp")),
        P(("section", "tp")),
    )
    return jax.shard_map(
        local,
        mesh=mesh,
        in_specs=placed,
        out_specs=(
            P("section", "grp", "tp"),
            P(None, "grp", ("section", "tp")),
            P(None, "grp", ("section", "tp")),
        ),
        check_vma=False,
    )
```

```python
import jax
import jax.numpy as jnp
from jax import lax
from jax.experimental import pallas as pl
from jax.experimental.pallas import tpu as pltpu
from jax.sharding import PartitionSpec as P

epsilon = 1e-06
MESH_AXES = ("section", "grp", "tp")


def shifts(mesh, along_x_core):
    n_sec, n_grp, n_tp = (mesh.shape[a] for a in MESH_AXES)
    n_x, n_y = n_tp // 2, 2 * n_sec

    def device(x, y, g):
        y_hi, y_lo = divmod(y % n_y, n_sec)
        return (y_lo * n_grp + g) * n_tp + (x % n_x) * 2 + y_hi

    def by(step):
        pairs = []
        for g in range(n_grp):
            dx, dy = (step, 0) if g % 2 == along_x_core else (0, step)
            for x in range(n_x):
                for y in range(n_y):
                    pairs.append((device(x, y, g), device(x + dx, y + dy, g)))
        return pairs

    return lambda value, step: lax.ppermute(value, MESH_AXES, by(step))


def cut_body(src, dst, sems):
    blocks, _, share = dst.shape
    copies = [pltpu.make_async_copy(src.at[:, pl.ds(i * share, share)], dst.at[i], sems.at[i]) for i in range(blocks)]
    for c in copies:
        c.start()
    for c in copies:
        c.wait()


def blocks_of_features(partial, blocks):
    rows, width = partial.shape
    return pl.pallas_call(
        cut_body,
        in_specs=[pl.BlockSpec(memory_space=pl.ANY)],
        out_specs=pl.BlockSpec(memory_space=pl.ANY),
        out_shape=jax.ShapeDtypeStruct((blocks, rows, width // blocks), partial.dtype),
        scratch_shapes=[pltpu.SemaphoreType.DMA((blocks,))],
        name="cut_features",
    )(partial)


def place_of(n):
    across = (0, -1, 1, -2)[n // 4]
    first = (0, -1, 1, 2)[n % 4]
    tp, section, core = lax.axis_index("tp"), lax.axis_index("section"), lax.axis_index("grp") % 2
    x = (tp // 2 + jnp.where(core == 0, across, first) + 4) % 4
    y = ((tp % 2) * 2 + section + jnp.where(core == 0, first, across) + 4) % 4
    return x * 2 + y // 2, y % 2


def prepare_body(gain, *refs):
    pairs, (scaled, root), squares = refs[:8], refs[8:10], refs[10]
    rows, share = pairs[0].shape[1:]
    squares[...] = jnp.zeros_like(squares)
    for n, pair in enumerate(pairs):
        for i in range(2):
            part, section = place_of(2 * n + i)
            hidden = pair[i].astype(jnp.float32)
            square = hidden * hidden
            lanes = square[:, :128]
            for c in range(1, share // 128):
                lanes += square[:, c * 128 : (c + 1) * 128]
            squares[section] += lanes
            scale = gain[part].astype(jnp.float32)
            scaled[part, section] = (hidden * scale).astype(jnp.bfloat16)
    width = share * scaled.shape[0]
    for s in range(2):
        mean_square = jnp.sum(squares[s], axis=-1, keepdims=True) / width
        root[s] = jnp.broadcast_to(lax.rsqrt(mean_square + epsilon), (rows, 128))


def prepare(gain, pairs, n_parts):
    rows, share = pairs[0].shape[1:]
    vmem = pl.BlockSpec(memory_space=pltpu.VMEM)
    return pl.pallas_call(
        prepare_body,
        in_specs=[vmem] * 9,
        out_specs=[vmem, vmem],
        out_shape=[
            jax.ShapeDtypeStruct((n_parts, 2, rows, share), jnp.bfloat16),
            jax.ShapeDtypeStruct((2, rows, 128), jnp.float32),
        ],
        scratch_shapes=[pltpu.VMEM((2, rows, 128), jnp.float32)],
        name="prepare",
    )(gain.reshape(n_parts, 1, share), *pairs)


def project_body(scaled, weights, root, bias_q, bias_kv, query, keyval, held_a, held_w, sems_a, sems_w):
    steps, rows, share = held_a.shape
    loads = []
    for k in range(steps):
        at = pl.ds(k * share, share)
        loads.append(pltpu.make_async_copy(weights.at[at, :], held_w.at[at, :], sems_w.at[k]))
        loads.append(pltpu.make_async_copy(scaled.at[k], held_a.at[k], sems_a.at[k]))
    for c in loads:
        c.start()
    total = None
    for k in range(steps):
        loads[2 * k].wait()
        loads[2 * k + 1].wait()
        term = jnp.dot(held_a[k], held_w[k * share : (k + 1) * share, :], preferred_element_type=jnp.float32)
        total = term if total is None else total + term
    split = query.shape[2]
    for s in range(2):
        half = total[s * rows // 2 : (s + 1) * rows // 2]
        scale = root[s][:, :1]
        query[s] = (half[:, :split] * scale + bias_q[...].astype(jnp.float32)).astype(query.dtype)
        keyval[s] = (half[:, split:] * scale + bias_kv[...].astype(jnp.float32)).astype(keyval.dtype)


def project(scaled, weights, root, bias_query, bias_keyval):
    steps, _, rows, share = scaled.shape
    width, cols = weights.shape
    q_cols = bias_query.shape[0]
    vmem, hbm = pl.BlockSpec(memory_space=pltpu.VMEM), pl.BlockSpec(memory_space=pl.ANY)
    return pl.pallas_call(
        project_body,
        in_specs=[hbm, hbm, vmem, vmem, vmem],
        out_specs=[vmem, vmem],
        out_shape=[
            jax.ShapeDtypeStruct((2, rows, q_cols), jnp.bfloat16),
            jax.ShapeDtypeStruct((2, rows, cols - q_cols), jnp.bfloat16),
        ],
        scratch_shapes=[
            pltpu.VMEM((steps, 2 * rows, share), jnp.bfloat16),
            pltpu.VMEM((width, cols), jnp.bfloat16),
            pltpu.SemaphoreType.DMA((steps,)),
            pltpu.SemaphoreType.DMA((steps,)),
        ],
        name="project",
    )(scaled.reshape(steps, 2 * rows, share), weights, root, bias_query[None, :], bias_keyval[None, :])


def solution(mesh):
    near = shifts(mesh, 1)
    across = shifts(mesh, 0)

    def local(partials, residual, norm_gain, w_query, w_keyval, bias_query, bias_keyval):
        weights = lax.all_gather(jnp.concatenate([w_query, w_keyval], axis=1), "grp", axis=0, tiled=True)
        n_tp = lax.axis_size("tp")
        cut = blocks_of_features(partials[0, 0], n_tp)
        arrived = lax.all_to_all(cut, "tp", split_axis=0, concat_axis=0, tiled=True)
        summed = arrived.astype(jnp.float32).sum(axis=0)
        hidden = (residual[0].astype(jnp.float32) + summed).astype(jnp.bfloat16)
        below, above, opposite = near(hidden, 1), near(hidden, -1), near(hidden, 2)
        one = jnp.stack([hidden, below])
        two = jnp.stack([above, opposite])
        one_below, two_above = across(one, 1), across(two, -1)
        one_above, two_below = across(one, -1), across(two, 1)
        one_opposite, two_opposite = across(one_below, 1), across(two_above, -1)
        pairs = [one, two, one_below, two_below, one_above, two_above, one_opposite, two_opposite]
        scaled, root = prepare(norm_gain, pairs, n_tp)
        query, keyval = project(scaled, weights, root, bias_query, bias_keyval)
        return hidden[None], query, keyval

    placed = (
        P("tp", "section", "grp", None),
        P("section", "grp", "tp"),
        P(),
        P("grp", ("section", "tp")),
        P("grp", ("section", "tp")),
        P(("section", "tp")),
        P(("section", "tp")),
    )
    return jax.shard_map(
        local,
        mesh=mesh,
        in_specs=placed,
        out_specs=(
            P("section", "grp", "tp"),
            P(None, "grp", ("section", "tp")),
            P(None, "grp", ("section", "tp")),
        ),
        check_vma=False,
    )
```

```python
import jax
import jax.numpy as jnp
from jax import lax
from jax.experimental import pallas as pl
from jax.experimental.pallas import tpu as pltpu
from jax.sharding import PartitionSpec as P

epsilon = 1e-06
MESH_AXES = ("section", "grp", "tp")


def shifts(mesh, along_x_core):
    n_sec, n_grp, n_tp = (mesh.shape[a] for a in MESH_AXES)
    n_x, n_y = n_tp // 2, 2 * n_sec

    def device(x, y, g):
        y_hi, y_lo = divmod(y % n_y, n_sec)
        return (y_lo * n_grp + g) * n_tp + (x % n_x) * 2 + y_hi

    def by(step):
        pairs = []
        for g in range(n_grp):
            dx, dy = (step, 0) if g % 2 == along_x_core else (0, step)
            for x in range(n_x):
                for y in range(n_y):
                    pairs.append((device(x, y, g), device(x + dx, y + dy, g)))
        return pairs

    return lambda value, step: lax.ppermute(value, MESH_AXES, by(step))


def cut_body(src, dst, sems):
    blocks, _, share = dst.shape
    copies = [pltpu.make_async_copy(src.at[:, pl.ds(i * share, share)], dst.at[i], sems.at[i]) for i in range(blocks)]
    for c in copies:
        c.start()
    for c in copies:
        c.wait()


def blocks_of_features(partial, blocks):
    rows, width = partial.shape
    return pl.pallas_call(
        cut_body,
        in_specs=[pl.BlockSpec(memory_space=pltpu.HBM)],
        out_specs=pl.BlockSpec(memory_space=pltpu.VMEM),
        out_shape=pltpu.VMEM((blocks, rows, width // blocks), partial.dtype),
        scratch_shapes=[pltpu.SemaphoreType.DMA((blocks,))],
        compiler_params=pltpu.CompilerParams(vmem_limit_bytes=8 << 20),
        name="cut_features",
    )(pltpu.with_memory_space_constraint(partial, pltpu.HBM))


def place_of(n):
    across = (0, -1, 1, -2)[n // 4]
    first = (0, -1, 1, 2)[n % 4]
    tp, section, core = lax.axis_index("tp"), lax.axis_index("section"), lax.axis_index("grp") % 2
    x = (tp // 2 + jnp.where(core == 0, across, first) + 4) % 4
    y = ((tp % 2) * 2 + section + jnp.where(core == 0, first, across) + 4) % 4
    return x * 2 + y // 2, y % 2


def prepare_body(gain, *refs):
    pairs, (scaled, root), squares = refs[:8], refs[8:10], refs[10]
    rows, share = pairs[0].shape[1:]
    squares[...] = jnp.zeros_like(squares)
    for n, pair in enumerate(pairs):
        for i in range(2):
            part, section = place_of(2 * n + i)
            hidden = pair[i].astype(jnp.float32)
            square = hidden * hidden
            lanes = square[:, :128]
            for c in range(1, share // 128):
                lanes += square[:, c * 128 : (c + 1) * 128]
            squares[section] += lanes
            scale = gain[part].astype(jnp.float32)
            scaled[part, section] = (hidden * scale).astype(jnp.bfloat16)
    width = share * scaled.shape[0]
    for s in range(2):
        mean_square = jnp.sum(squares[s], axis=-1, keepdims=True) / width
        root[s] = jnp.broadcast_to(lax.rsqrt(mean_square + epsilon), (rows, 128))


def prepare(gain, pairs, n_parts):
    rows, share = pairs[0].shape[1:]
    vmem = pl.BlockSpec(memory_space=pltpu.VMEM)
    return pl.pallas_call(
        prepare_body,
        in_specs=[vmem] * 9,
        out_specs=[vmem, vmem],
        out_shape=[
            pltpu.VMEM((n_parts, 2, rows, share), jnp.bfloat16),
            pltpu.VMEM((2, rows, 128), jnp.float32),
        ],
        scratch_shapes=[pltpu.VMEM((2, rows, 128), jnp.float32)],
        compiler_params=pltpu.CompilerParams(vmem_limit_bytes=24 << 20),
        name="prepare",
    )(gain.reshape(n_parts, 1, share), *[pltpu.with_memory_space_constraint(p, pltpu.VMEM) for p in pairs])


def project_body(scaled, weights, root, bias_q, bias_kv, query, keyval, held_a, held_w, sems):
    steps, rows, share = held_a.shape
    ahead = 3

    def load(k):
        at = pl.ds(k * share, share)
        return (
            pltpu.make_async_copy(scaled.at[k], held_a.at[k], sems.at[0, k]),
            pltpu.make_async_copy(weights.at[at, :], held_w.at[at, :], sems.at[1, k]),
        )

    loads = [load(k) for k in range(steps)]
    for k in range(ahead):
        for c in loads[k]:
            c.start()
    total = None
    for k in range(steps):
        for c in loads[k]:
            c.wait()
        if k + ahead < steps:
            for c in loads[k + ahead]:
                c.start()
        term = jnp.dot(held_a[k], held_w[k * share : (k + 1) * share, :], preferred_element_type=jnp.float32)
        total = term if total is None else total + term
    split = query.shape[2]
    for s in range(2):
        half = total[s * rows // 2 : (s + 1) * rows // 2]
        scale = root[s][:, :1]
        query[s] = (half[:, :split] * scale + bias_q[...].astype(jnp.float32)).astype(query.dtype)
        keyval[s] = (half[:, split:] * scale + bias_kv[...].astype(jnp.float32)).astype(keyval.dtype)


def project(scaled, weights, root, bias_query, bias_keyval):
    steps, _, rows, share = scaled.shape
    width, cols = weights.shape
    scaled = pltpu.with_memory_space_constraint(scaled.reshape(steps, 2 * rows, share), pltpu.HBM)
    q_cols = bias_query.shape[0]
    vmem, hbm = pl.BlockSpec(memory_space=pltpu.VMEM), pl.BlockSpec(memory_space=pltpu.HBM)
    return pl.pallas_call(
        project_body,
        in_specs=[hbm, hbm, vmem, vmem, vmem],
        out_specs=[vmem, vmem],
        out_shape=[
            jax.ShapeDtypeStruct((2, rows, q_cols), jnp.bfloat16),
            jax.ShapeDtypeStruct((2, rows, cols - q_cols), jnp.bfloat16),
        ],
        scratch_shapes=[
            pltpu.VMEM((steps, 2 * rows, share), jnp.bfloat16),
            pltpu.VMEM((width, cols), jnp.bfloat16),
            pltpu.SemaphoreType.DMA((2, steps)),
        ],
        compiler_params=pltpu.CompilerParams(vmem_limit_bytes=32 << 20),
        name="project",
    )(scaled, pltpu.with_memory_space_constraint(weights, pltpu.HBM), root, bias_query[None, :], bias_keyval[None, :])


def solution(mesh):
    near = shifts(mesh, 1)
    across = shifts(mesh, 0)

    def local(partials, residual, norm_gain, w_query, w_keyval, bias_query, bias_keyval):
        weights = lax.all_gather(jnp.concatenate([w_query, w_keyval], axis=1), "grp", axis=0, tiled=True)
        n_tp = lax.axis_size("tp")
        cut = blocks_of_features(partials[0, 0], n_tp)
        arrived = lax.all_to_all(cut, "tp", split_axis=0, concat_axis=0, tiled=True)
        summed = arrived.astype(jnp.float32).sum(axis=0)
        hidden = (residual[0].astype(jnp.float32) + summed).astype(jnp.bfloat16)
        below, above, opposite = near(hidden, 1), near(hidden, -1), near(hidden, 2)
        one = jnp.stack([hidden, below])
        two = jnp.stack([above, opposite])
        one_below, two_above = across(one, 1), across(two, -1)
        one_above, two_below = across(one, -1), across(two, 1)
        one_opposite, two_opposite = across(one_below, 1), across(two_above, -1)
        pairs = [one, two, one_below, two_below, one_above, two_above, one_opposite, two_opposite]
        scaled, root = prepare(norm_gain, pairs, n_tp)
        query, keyval = project(scaled, weights, root, bias_query, bias_keyval)
        return hidden[None], query, keyval

    placed = (
        P("tp", "section", "grp", None),
        P("section", "grp", "tp"),
        P(),
        P("grp", ("section", "tp")),
        P("grp", ("section", "tp")),
        P(("section", "tp")),
        P(("section", "tp")),
    )
    return jax.shard_map(
        local,
        mesh=mesh,
        in_specs=placed,
        out_specs=(
            P("section", "grp", "tp"),
            P(None, "grp", ("section", "tp")),
            P(None, "grp", ("section", "tp")),
        ),
        check_vma=False,
    )
```

```python
import jax
import jax.numpy as jnp
from jax import lax
from jax.experimental import pallas as pl
from jax.experimental.pallas import tpu as pltpu
from jax.sharding import PartitionSpec as P

epsilon = 1e-06
MESH_AXES = ("section", "grp", "tp")


def shifts(mesh, along_x_core):
    n_sec, n_grp, n_tp = (mesh.shape[a] for a in MESH_AXES)
    n_x, n_y = n_tp // 2, 2 * n_sec

    def device(x, y, g):
        y_hi, y_lo = divmod(y % n_y, n_sec)
        return (y_lo * n_grp + g) * n_tp + (x % n_x) * 2 + y_hi

    def by(step):
        pairs = []
        for g in range(n_grp):
            dx, dy = (step, 0) if g % 2 == along_x_core else (0, step)
            for x in range(n_x):
                for y in range(n_y):
                    pairs.append((device(x, y, g), device(x + dx, y + dy, g)))
        return pairs

    return lambda value, step: lax.ppermute(value, MESH_AXES, by(step))


def cut_body(src, dst, sems):
    blocks, _, share = dst.shape
    copies = [pltpu.make_async_copy(src.at[:, pl.ds(i * share, share)], dst.at[i], sems.at[i]) for i in range(blocks)]
    for c in copies:
        c.start()
    for c in copies:
        c.wait()


def join_body(one, two, dst, sems):
    width = one.shape[1]
    copies = [
        pltpu.make_async_copy(one, dst.at[:, pl.ds(0, width)], sems.at[0]),
        pltpu.make_async_copy(two, dst.at[:, pl.ds(width, two.shape[1])], sems.at[1]),
    ]
    for c in copies:
        c.start()
    for c in copies:
        c.wait()


def joined(one, two):
    hbm = pl.BlockSpec(memory_space=pltpu.HBM)
    return pl.pallas_call(
        join_body,
        in_specs=[hbm, hbm],
        out_specs=pl.BlockSpec(memory_space=pltpu.VMEM),
        out_shape=pltpu.VMEM((one.shape[0], one.shape[1] + two.shape[1]), one.dtype),
        scratch_shapes=[pltpu.SemaphoreType.DMA((2,))],
        compiler_params=pltpu.CompilerParams(vmem_limit_bytes=8 << 20),
        name="join_weights",
    )(*[pltpu.with_memory_space_constraint(w, pltpu.HBM) for w in (one, two)])


def blocks_of_features(partial, blocks):
    rows, width = partial.shape
    return pl.pallas_call(
        cut_body,
        in_specs=[pl.BlockSpec(memory_space=pltpu.HBM)],
        out_specs=pl.BlockSpec(memory_space=pltpu.VMEM),
        out_shape=pltpu.VMEM((blocks, rows, width // blocks), partial.dtype),
        scratch_shapes=[pltpu.SemaphoreType.DMA((blocks,))],
        compiler_params=pltpu.CompilerParams(vmem_limit_bytes=8 << 20),
        name="cut_features",
    )(pltpu.with_memory_space_constraint(partial, pltpu.HBM))


def place_of(n):
    across = (0, -1, 1, -2)[n // 4]
    first = (0, -1, 1, 2)[n % 4]
    tp, section, core = lax.axis_index("tp"), lax.axis_index("section"), lax.axis_index("grp") % 2
    x = (tp // 2 + jnp.where(core == 0, across, first) + 4) % 4
    y = ((tp % 2) * 2 + section + jnp.where(core == 0, first, across) + 4) % 4
    return x * 2 + y // 2, y % 2


def prepare_body(gain, *refs):
    pairs, (scaled, root), squares = refs[:8], refs[8:10], refs[10]
    rows, share = pairs[0].shape[1:]
    squares[...] = jnp.zeros_like(squares)
    for n, pair in enumerate(pairs):
        for i in range(2):
            part, section = place_of(2 * n + i)
            hidden = pair[i].astype(jnp.float32)
            square = hidden * hidden
            lanes = square[:, :128]
            for c in range(1, share // 128):
                lanes += square[:, c * 128 : (c + 1) * 128]
            squares[section] += lanes
            scale = gain[part].astype(jnp.float32)
            at = pl.multiple_of((part % 2) * share, share)
            scaled[part // 2, section, :, pl.ds(at, share)] = (hidden * scale).astype(jnp.bfloat16)
    width = share * gain.shape[0]
    for s in range(2):
        mean_square = jnp.sum(squares[s], axis=-1, keepdims=True) / width
        root[s] = jnp.broadcast_to(lax.rsqrt(mean_square + epsilon), (rows, 128))


def prepare(gain, pairs, n_parts):
    rows, share = pairs[0].shape[1:]
    vmem = pl.BlockSpec(memory_space=pltpu.VMEM)
    return pl.pallas_call(
        prepare_body,
        in_specs=[vmem] * 9,
        out_specs=[vmem, vmem],
        out_shape=[
            pltpu.VMEM((n_parts // 2, 2, rows, 2 * share), jnp.bfloat16),
            pltpu.VMEM((2, rows, 128), jnp.float32),
        ],
        scratch_shapes=[pltpu.VMEM((2, rows, 128), jnp.float32)],
        compiler_params=pltpu.CompilerParams(vmem_limit_bytes=24 << 20),
        name="prepare",
    )(gain.reshape(n_parts, 1, share), *[pltpu.with_memory_space_constraint(p, pltpu.VMEM) for p in pairs])


def project_body(scaled, weights, root, bias_q, bias_kv, query, keyval, held_a, held_w, total, sems):
    steps, rows, share = held_a.shape
    loads = []
    for k in range(steps):
        at = pl.ds(k * share, share)
        loads.append(pltpu.make_async_copy(scaled.at[k], held_a.at[k], sems.at[0, k]))
        loads.append(pltpu.make_async_copy(weights.at[at, :], held_w.at[at, :], sems.at[1, k]))
    for c in loads:
        c.start()
    for k in range(steps):
        loads[2 * k].wait()
        loads[2 * k + 1].wait()
        term = jnp.dot(held_a[k], held_w[k * share : (k + 1) * share, :], preferred_element_type=jnp.float32)
        if k == 0:
            total[...] = term
        elif k < steps - 1:
            total[...] += term
    term = total[...] + term
    split = query.shape[2]
    for s in range(2):
        half = term[s * rows // 2 : (s + 1) * rows // 2]
        scale = root[s][:, :1]
        query[s] = (half[:, :split] * scale + bias_q[...].astype(jnp.float32)).astype(query.dtype)
        keyval[s] = (half[:, split:] * scale + bias_kv[...].astype(jnp.float32)).astype(keyval.dtype)


def project(scaled, weights, root, bias_query, bias_keyval):
    steps, _, rows, share = scaled.shape
    width, cols = weights.shape
    scaled = pltpu.with_memory_space_constraint(scaled.reshape(steps, 2 * rows, share), pltpu.HBM)
    q_cols = bias_query.shape[0]
    vmem, hbm = pl.BlockSpec(memory_space=pltpu.VMEM), pl.BlockSpec(memory_space=pltpu.HBM)
    return pl.pallas_call(
        project_body,
        in_specs=[hbm, hbm, vmem, vmem, vmem],
        out_specs=[vmem, vmem],
        out_shape=[
            jax.ShapeDtypeStruct((2, rows, q_cols), jnp.bfloat16),
            jax.ShapeDtypeStruct((2, rows, cols - q_cols), jnp.bfloat16),
        ],
        scratch_shapes=[
            pltpu.VMEM((steps, 2 * rows, share), jnp.bfloat16),
            pltpu.VMEM((width, cols), jnp.bfloat16),
            pltpu.VMEM((2 * rows, cols), jnp.float32),
            pltpu.SemaphoreType.DMA((2, steps)),
        ],
        compiler_params=pltpu.CompilerParams(vmem_limit_bytes=32 << 20),
        name="project",
    )(scaled, pltpu.with_memory_space_constraint(weights, pltpu.HBM), root, bias_query[None, :], bias_keyval[None, :])


def solution(mesh):
    near = shifts(mesh, 1)
    across = shifts(mesh, 0)

    def local(partials, residual, norm_gain, w_query, w_keyval, bias_query, bias_keyval):
        weights = lax.all_gather(joined(w_query, w_keyval), "grp", axis=0, tiled=True)
        n_tp = lax.axis_size("tp")
        cut = blocks_of_features(partials[0, 0], n_tp)
        arrived = lax.all_to_all(cut, "tp", split_axis=0, concat_axis=0, tiled=True)
        summed = arrived.astype(jnp.float32).sum(axis=0)
        hidden = (residual[0].astype(jnp.float32) + summed).astype(jnp.bfloat16)
        below, above, opposite = near(hidden, 1), near(hidden, -1), near(hidden, 2)
        one = jnp.stack([hidden, below])
        two = jnp.stack([above, opposite])
        one_below, two_above = across(one, 1), across(two, -1)
        one_above, two_below = across(one, -1), across(two, 1)
        one_opposite, two_opposite = across(one_below, 1), across(two_above, -1)
        pairs = [one, two, one_below, two_below, one_above, two_above, one_opposite, two_opposite]
        scaled, root = prepare(norm_gain, pairs, n_tp)
        query, keyval = project(scaled, weights, root, bias_query, bias_keyval)
        return hidden[None], query, keyval

    placed = (
        P("tp", "section", "grp", None),
        P("section", "grp", "tp"),
        P(),
        P("grp", ("section", "tp")),
        P("grp", ("section", "tp")),
        P(("section", "tp")),
        P(("section", "tp")),
    )
    return jax.shard_map(
        local,
        mesh=mesh,
        in_specs=placed,
        out_specs=(
            P("section", "grp", "tp"),
            P(None, "grp", ("section", "tp")),
            P(None, "grp", ("section", "tp")),
        ),
        check_vma=False,
    )
```

```python
import jax
import jax.numpy as jnp
from jax import lax
from jax.experimental import pallas as pl
from jax.experimental.pallas import tpu as pltpu
from jax.sharding import PartitionSpec as P

epsilon = 1e-06
MESH_AXES = ("section", "grp", "tp")


def shifts(mesh, along_x_core):
    n_sec, n_grp, n_tp = (mesh.shape[a] for a in MESH_AXES)
    n_x, n_y = n_tp // 2, 2 * n_sec

    def device(x, y, g):
        y_hi, y_lo = divmod(y % n_y, n_sec)
        return (y_lo * n_grp + g) * n_tp + (x % n_x) * 2 + y_hi

    def by(step):
        pairs = []
        for g in range(n_grp):
            dx, dy = (step, 0) if g % 2 == along_x_core else (0, step)
            for x in range(n_x):
                for y in range(n_y):
                    pairs.append((device(x, y, g), device(x + dx, y + dy, g)))
        return pairs

    return lambda value, step: lax.ppermute(value, MESH_AXES, by(step))


def cut_body(src, dst, sems):
    blocks, _, share = dst.shape
    copies = [pltpu.make_async_copy(src.at[:, pl.ds(i * share, share)], dst.at[i], sems.at[i]) for i in range(blocks)]
    for c in copies:
        c.start()
    for c in copies:
        c.wait()


def join_body(one, two, dst, sems):
    width = one.shape[1]
    copies = [
        pltpu.make_async_copy(one, dst.at[:, pl.ds(0, width)], sems.at[0]),
        pltpu.make_async_copy(two, dst.at[:, pl.ds(width, two.shape[1])], sems.at[1]),
    ]
    for c in copies:
        c.start()
    for c in copies:
        c.wait()


def joined(one, two):
    hbm = pl.BlockSpec(memory_space=pltpu.HBM)
    return pl.pallas_call(
        join_body,
        in_specs=[hbm, hbm],
        out_specs=pl.BlockSpec(memory_space=pltpu.VMEM),
        out_shape=pltpu.VMEM((one.shape[0], one.shape[1] + two.shape[1]), one.dtype),
        scratch_shapes=[pltpu.SemaphoreType.DMA((2,))],
        compiler_params=pltpu.CompilerParams(vmem_limit_bytes=8 << 20),
        name="join_weights",
    )(*[pltpu.with_memory_space_constraint(w, pltpu.HBM) for w in (one, two)])


def blocks_of_features(partial, blocks):
    rows, width = partial.shape
    return pl.pallas_call(
        cut_body,
        in_specs=[pl.BlockSpec(memory_space=pltpu.HBM)],
        out_specs=pl.BlockSpec(memory_space=pltpu.VMEM),
        out_shape=pltpu.VMEM((blocks, rows, width // blocks), partial.dtype),
        scratch_shapes=[pltpu.SemaphoreType.DMA((blocks,))],
        compiler_params=pltpu.CompilerParams(vmem_limit_bytes=8 << 20),
        name="cut_features",
    )(pltpu.with_memory_space_constraint(partial, pltpu.HBM))


def place_of(n):
    across = (0, -1, 1, -2)[n // 4]
    first = (0, -1, 1, 2)[n % 4]
    tp, section, core = lax.axis_index("tp"), lax.axis_index("section"), lax.axis_index("grp") % 2
    x = (tp // 2 + jnp.where(core == 0, across, first) + 4) % 4
    y = ((tp % 2) * 2 + section + jnp.where(core == 0, first, across) + 4) % 4
    return x * 2 + y // 2, y % 2


def prepare_body(gain, *refs):
    pairs, (scaled, root), squares = refs[:8], refs[8:10], refs[10]
    rows, share = pairs[0].shape[1:]
    squares[...] = jnp.zeros_like(squares)
    for n, pair in enumerate(pairs):
        for i in range(2):
            part, section = place_of(2 * n + i)
            hidden = pair[i].astype(jnp.float32)
            square = hidden * hidden
            lanes = square[:, :128]
            for c in range(1, share // 128):
                lanes += square[:, c * 128 : (c + 1) * 128]
            squares[section] += lanes
            scale = gain[part].astype(jnp.float32)
            at = pl.multiple_of((part % 2) * share, share)
            scaled[part // 2, section, :, pl.ds(at, share)] = (hidden * scale).astype(jnp.bfloat16)
    width = share * gain.shape[0]
    for s in range(2):
        mean_square = jnp.sum(squares[s], axis=-1, keepdims=True) / width
        root[s] = jnp.broadcast_to(lax.rsqrt(mean_square + epsilon), (rows, 128))


def prepare(gain, pairs, n_parts):
    rows, share = pairs[0].shape[1:]
    vmem = pl.BlockSpec(memory_space=pltpu.VMEM)
    return pl.pallas_call(
        prepare_body,
        in_specs=[vmem] * 9,
        out_specs=[vmem, vmem],
        out_shape=[
            pltpu.VMEM((n_parts // 2, 2, rows, 2 * share), jnp.bfloat16),
            pltpu.VMEM((2, rows, 128), jnp.float32),
        ],
        scratch_shapes=[pltpu.VMEM((2, rows, 128), jnp.float32)],
        compiler_params=pltpu.CompilerParams(vmem_limit_bytes=24 << 20),
        name="prepare",
    )(gain.reshape(n_parts, 1, share), *[pltpu.with_memory_space_constraint(p, pltpu.VMEM) for p in pairs])


def hold_body(scaled, held, rest):
    kept = held.shape[0]
    for k in range(kept):
        held[k] = scaled[k]
    for k in range(rest.shape[0]):
        rest[k] = scaled[kept + k]


def hold(scaled, kept):
    vmem = pl.BlockSpec(memory_space=pltpu.VMEM)
    steps, *block = scaled.shape
    return pl.pallas_call(
        hold_body,
        in_specs=[vmem],
        out_specs=[vmem, vmem],
        out_shape=[
            pltpu.VMEM((kept, *block), scaled.dtype),
            jax.ShapeDtypeStruct((steps - kept, *block), scaled.dtype),
        ],
        compiler_params=pltpu.CompilerParams(vmem_limit_bytes=16 << 20),
        name="hold",
    )(pltpu.with_memory_space_constraint(scaled, pltpu.VMEM))


def project_body(scaled, rest, weights, root, bias_q, bias_kv, query, keyval, held_a, held_w, total, sems_a, sems_w):
    kept, rows, share = scaled.shape
    steps = kept + rest.shape[0]
    loads = []
    for k in range(steps):
        at = pl.ds(k * share, share)
        loads.append(pltpu.make_async_copy(weights.at[at, :], held_w.at[at, :], sems_w.at[k]))
    late = [pltpu.make_async_copy(rest.at[k], held_a.at[k], sems_a.at[k]) for k in range(steps - kept)]
    for c in loads + late:
        c.start()
    for k in range(steps):
        loads[k].wait()
        if k >= kept:
            late[k - kept].wait()
        left = scaled[k] if k < kept else held_a[k - kept]
        term = jnp.dot(left, held_w[k * share : (k + 1) * share, :], preferred_element_type=jnp.float32)
        if k == 0:
            total[...] = term
        elif k < steps - 1:
            total[...] += term
    term = total[...] + term
    split = query.shape[2]
    for s in range(2):
        half = term[s * rows // 2 : (s + 1) * rows // 2]
        scale = root[s][:, :1]
        query[s] = (half[:, :split] * scale + bias_q[...].astype(jnp.float32)).astype(query.dtype)
        keyval[s] = (half[:, split:] * scale + bias_kv[...].astype(jnp.float32)).astype(keyval.dtype)


def project(scaled, weights, root, bias_query, bias_keyval):
    steps, _, rows, share = scaled.shape
    width, cols = weights.shape
    kept = steps - 1
    scaled, rest = hold(scaled.reshape(steps, 2 * rows, share), kept)
    scaled = pltpu.with_memory_space_constraint(scaled, pltpu.VMEM)
    rest = pltpu.with_memory_space_constraint(rest, pltpu.HBM)
    q_cols = bias_query.shape[0]
    vmem, hbm = pl.BlockSpec(memory_space=pltpu.VMEM), pl.BlockSpec(memory_space=pltpu.HBM)
    return pl.pallas_call(
        project_body,
        in_specs=[vmem, hbm, hbm, vmem, vmem, vmem],
        out_specs=[vmem, vmem],
        out_shape=[
            jax.ShapeDtypeStruct((2, rows, q_cols), jnp.bfloat16),
            jax.ShapeDtypeStruct((2, rows, cols - q_cols), jnp.bfloat16),
        ],
        scratch_shapes=[
            pltpu.VMEM((steps - kept, 2 * rows, share), jnp.bfloat16),
            pltpu.VMEM((width, cols), jnp.bfloat16),
            pltpu.VMEM((2 * rows, cols), jnp.float32),
            pltpu.SemaphoreType.DMA((steps - kept,)),
            pltpu.SemaphoreType.DMA((steps,)),
        ],
        compiler_params=pltpu.CompilerParams(vmem_limit_bytes=24 << 20),
        name="project",
    )(scaled, rest, pltpu.with_memory_space_constraint(weights, pltpu.HBM), root, bias_query[None, :], bias_keyval[None, :])


def solution(mesh):
    near = shifts(mesh, 1)
    across = shifts(mesh, 0)

    def local(partials, residual, norm_gain, w_query, w_keyval, bias_query, bias_keyval):
        weights = lax.all_gather(joined(w_query, w_keyval), "grp", axis=0, tiled=True)
        n_tp = lax.axis_size("tp")
        cut = blocks_of_features(partials[0, 0], n_tp)
        arrived = lax.all_to_all(cut, "tp", split_axis=0, concat_axis=0, tiled=True)
        summed = arrived.astype(jnp.float32).sum(axis=0)
        hidden = (residual[0].astype(jnp.float32) + summed).astype(jnp.bfloat16)
        below, above, opposite = near(hidden, 1), near(hidden, -1), near(hidden, 2)
        one = jnp.stack([hidden, below])
        two = jnp.stack([above, opposite])
        one_below, two_above = across(one, 1), across(two, -1)
        one_above, two_below = across(one, -1), across(two, 1)
        one_opposite, two_opposite = across(one_below, 1), across(two_above, -1)
        pairs = [one, two, one_below, two_below, one_above, two_above, one_opposite, two_opposite]
        scaled, root = prepare(norm_gain, pairs, n_tp)
        query, keyval = project(scaled, weights, root, bias_query, bias_keyval)
        return hidden[None], query, keyval

    placed = (
        P("tp", "section", "grp", None),
        P("section", "grp", "tp"),
        P(),
        P("grp", ("section", "tp")),
        P("grp", ("section", "tp")),
        P(("section", "tp")),
        P(("section", "tp")),
    )
    return jax.shard_map(
        local,
        mesh=mesh,
        in_specs=placed,
        out_specs=(
            P("section", "grp", "tp"),
            P(None, "grp", ("section", "tp")),
            P(None, "grp", ("section", "tp")),
        ),
        check_vma=False,
    )
```

```python
import jax
import jax.numpy as jnp
from jax import lax
from jax.experimental import pallas as pl
from jax.experimental.pallas import tpu as pltpu
from jax.sharding import PartitionSpec as P

epsilon = 1e-06
MESH_AXES = ("section", "grp", "tp")


def shifts(mesh, along_x_core):
    n_sec, n_grp, n_tp = (mesh.shape[a] for a in MESH_AXES)
    n_x, n_y = n_tp // 2, 2 * n_sec

    def device(x, y, g):
        y_hi, y_lo = divmod(y % n_y, n_sec)
        return (y_lo * n_grp + g) * n_tp + (x % n_x) * 2 + y_hi

    def by(step):
        pairs = []
        for g in range(n_grp):
            dx, dy = (step, 0) if g % 2 == along_x_core else (0, step)
            for x in range(n_x):
                for y in range(n_y):
                    pairs.append((device(x, y, g), device(x + dx, y + dy, g)))
        return pairs

    return lambda value, step: lax.ppermute(value, MESH_AXES, by(step))


def cut_body(src, dst, sems):
    blocks, _, share = dst.shape
    copies = [pltpu.make_async_copy(src.at[:, pl.ds(i * share, share)], dst.at[i], sems.at[i]) for i in range(blocks)]
    for c in copies:
        c.start()
    for c in copies:
        c.wait()


def join_body(one, two, dst, held, sems, out_sems):
    rows, width = one.shape
    chunks = out_sems.shape[0]
    share = rows // chunks
    loads, stores = [], []
    for k in range(chunks):
        at = pl.ds(k * share, share)
        left, right = held.at[at, pl.ds(0, width)], held.at[at, pl.ds(width, two.shape[1])]
        loads.append(pltpu.make_async_copy(one.at[at, :], left, sems.at[0, k]))
        loads.append(pltpu.make_async_copy(two.at[at, :], right, sems.at[1, k]))
        stores.append(pltpu.make_async_copy(held.at[at, :], dst.at[at, :], out_sems.at[k]))
    for c in loads:
        c.start()
    for k in range(chunks):
        loads[2 * k].wait()
        loads[2 * k + 1].wait()
        stores[k].start()
    for c in stores:
        c.wait()


def joined(one, two):
    hbm = pl.BlockSpec(memory_space=pltpu.HBM)
    shape = (one.shape[0], one.shape[1] + two.shape[1])
    return pl.pallas_call(
        join_body,
        in_specs=[hbm, hbm],
        out_specs=hbm,
        out_shape=jax.ShapeDtypeStruct(shape, one.dtype),
        scratch_shapes=[
            pltpu.VMEM(shape, one.dtype),
            pltpu.SemaphoreType.DMA((2, 4)),
            pltpu.SemaphoreType.DMA((4,)),
        ],
        compiler_params=pltpu.CompilerParams(vmem_limit_bytes=8 << 20),
        name="join_weights",
    )(*[pltpu.with_memory_space_constraint(w, pltpu.HBM) for w in (one, two)])


def blocks_of_features(partial, blocks):
    rows, width = partial.shape
    return pl.pallas_call(
        cut_body,
        in_specs=[pl.BlockSpec(memory_space=pltpu.HBM)],
        out_specs=pl.BlockSpec(memory_space=pltpu.VMEM),
        out_shape=pltpu.VMEM((blocks, rows, width // blocks), partial.dtype),
        scratch_shapes=[pltpu.SemaphoreType.DMA((blocks,))],
        compiler_params=pltpu.CompilerParams(vmem_limit_bytes=8 << 20),
        name="cut_features",
    )(pltpu.with_memory_space_constraint(partial, pltpu.HBM))


def place_of(n):
    across = (0, -1, 1, -2)[n // 4]
    first = (0, -1, 1, 2)[n % 4]
    tp, section, core = lax.axis_index("tp"), lax.axis_index("section"), lax.axis_index("grp") % 2
    x = (tp // 2 + jnp.where(core == 0, across, first) + 4) % 4
    y = ((tp % 2) * 2 + section + jnp.where(core == 0, first, across) + 4) % 4
    return x * 2 + y // 2, y % 2


def prepare_body(gain, *refs):
    pairs, (scaled, root), squares = refs[:8], refs[8:10], refs[10]
    rows, share = pairs[0].shape[1:]
    squares[...] = jnp.zeros_like(squares)
    for n, pair in enumerate(pairs):
        for i in range(2):
            part, section = place_of(2 * n + i)
            hidden = pair[i].astype(jnp.float32)
            square = hidden * hidden
            lanes = square[:, :128]
            for c in range(1, share // 128):
                lanes += square[:, c * 128 : (c + 1) * 128]
            squares[section] += lanes
            scale = gain[part].astype(jnp.float32)
            at = pl.multiple_of((part % 2) * share, share)
            scaled[part // 2, section, :, pl.ds(at, share)] = (hidden * scale).astype(jnp.bfloat16)
    width = share * gain.shape[0]
    for s in range(2):
        mean_square = jnp.sum(squares[s], axis=-1, keepdims=True) / width
        root[s] = jnp.broadcast_to(lax.rsqrt(mean_square + epsilon), (rows, 128))


def prepare(gain, pairs, n_parts):
    rows, share = pairs[0].shape[1:]
    vmem = pl.BlockSpec(memory_space=pltpu.VMEM)
    return pl.pallas_call(
        prepare_body,
        in_specs=[vmem] * 9,
        out_specs=[vmem, vmem],
        out_shape=[
            pltpu.VMEM((n_parts // 2, 2, rows, 2 * share), jnp.bfloat16),
            pltpu.VMEM((2, rows, 128), jnp.float32),
        ],
        scratch_shapes=[pltpu.VMEM((2, rows, 128), jnp.float32)],
        compiler_params=pltpu.CompilerParams(vmem_limit_bytes=24 << 20),
        name="prepare",
    )(gain.reshape(n_parts, 1, share), *[pltpu.with_memory_space_constraint(p, pltpu.VMEM) for p in pairs])


def hold_body(scaled, held, rest):
    kept = held.shape[0]
    for k in range(kept):
        held[k] = scaled[k]
    for k in range(rest.shape[0]):
        rest[k] = scaled[kept + k]


def hold(scaled, kept):
    vmem = pl.BlockSpec(memory_space=pltpu.VMEM)
    steps, *block = scaled.shape
    return pl.pallas_call(
        hold_body,
        in_specs=[vmem],
        out_specs=[vmem, vmem],
        out_shape=[
            pltpu.VMEM((kept, *block), scaled.dtype),
            jax.ShapeDtypeStruct((steps - kept, *block), scaled.dtype),
        ],
        compiler_params=pltpu.CompilerParams(vmem_limit_bytes=16 << 20),
        name="hold",
    )(pltpu.with_memory_space_constraint(scaled, pltpu.VMEM))


def project_body(scaled, rest, weights, root, bias_q, bias_kv, query, keyval, held_a, held_w, total, sems_a, sems_w):
    kept, rows, share = scaled.shape
    steps = kept + rest.shape[0]
    loads = []
    for k in range(steps):
        at = pl.ds(k * share, share)
        loads.append(pltpu.make_async_copy(weights.at[at, :], held_w.at[at, :], sems_w.at[k]))
    late = [pltpu.make_async_copy(rest.at[k], held_a.at[k], sems_a.at[k]) for k in range(steps - kept)]
    for c in loads + late:
        c.start()
    for k in range(steps):
        loads[k].wait()
        if k >= kept:
            late[k - kept].wait()
        left = scaled[k] if k < kept else held_a[k - kept]
        term = jnp.dot(left, held_w[k * share : (k + 1) * share, :], preferred_element_type=jnp.float32)
        if k == 0:
            total[...] = term
        elif k < steps - 1:
            total[...] += term
    term = total[...] + term
    split = query.shape[2]
    for s in range(2):
        half = term[s * rows // 2 : (s + 1) * rows // 2]
        scale = root[s][:, :1]
        query[s] = (half[:, :split] * scale + bias_q[...].astype(jnp.float32)).astype(query.dtype)
        keyval[s] = (half[:, split:] * scale + bias_kv[...].astype(jnp.float32)).astype(keyval.dtype)


def project(scaled, weights, root, bias_query, bias_keyval):
    steps, _, rows, share = scaled.shape
    width, cols = weights.shape
    kept = steps - 1
    scaled, rest = hold(scaled.reshape(steps, 2 * rows, share), kept)
    scaled = pltpu.with_memory_space_constraint(scaled, pltpu.VMEM)
    rest = pltpu.with_memory_space_constraint(rest, pltpu.HBM)
    q_cols = bias_query.shape[0]
    vmem, hbm = pl.BlockSpec(memory_space=pltpu.VMEM), pl.BlockSpec(memory_space=pltpu.HBM)
    return pl.pallas_call(
        project_body,
        in_specs=[vmem, hbm, hbm, vmem, vmem, vmem],
        out_specs=[vmem, vmem],
        out_shape=[
            jax.ShapeDtypeStruct((2, rows, q_cols), jnp.bfloat16),
            jax.ShapeDtypeStruct((2, rows, cols - q_cols), jnp.bfloat16),
        ],
        scratch_shapes=[
            pltpu.VMEM((steps - kept, 2 * rows, share), jnp.bfloat16),
            pltpu.VMEM((width, cols), jnp.bfloat16),
            pltpu.VMEM((2 * rows, cols), jnp.float32),
            pltpu.SemaphoreType.DMA((steps - kept,)),
            pltpu.SemaphoreType.DMA((steps,)),
        ],
        compiler_params=pltpu.CompilerParams(vmem_limit_bytes=24 << 20),
        name="project",
    )(scaled, rest, pltpu.with_memory_space_constraint(weights, pltpu.HBM), root, bias_query[None, :], bias_keyval[None, :])


def solution(mesh):
    near = shifts(mesh, 1)
    across = shifts(mesh, 0)

    def local(partials, residual, norm_gain, w_query, w_keyval, bias_query, bias_keyval):
        weights = lax.all_gather(joined(w_query, w_keyval), "grp", axis=0, tiled=True)
        n_tp = lax.axis_size("tp")
        cut = blocks_of_features(partials[0, 0], n_tp)
        arrived = lax.all_to_all(cut, "tp", split_axis=0, concat_axis=0, tiled=True)
        summed = arrived.astype(jnp.float32).sum(axis=0)
        hidden = (residual[0].astype(jnp.float32) + summed).astype(jnp.bfloat16)
        below, above, opposite = near(hidden, 1), near(hidden, -1), near(hidden, 2)
        one = jnp.stack([hidden, below])
        two = jnp.stack([above, opposite])
        one_below, two_above = across(one, 1), across(two, -1)
        one_above, two_below = across(one, -1), across(two, 1)
        one_opposite, two_opposite = across(one_below, 1), across(two_above, -1)
        pairs = [one, two, one_below, two_below, one_above, two_above, one_opposite, two_opposite]
        scaled, root = prepare(norm_gain, pairs, n_tp)
        query, keyval = project(scaled, weights, root, bias_query, bias_keyval)
        return hidden[None], query, keyval

    placed = (
        P("tp", "section", "grp", None),
        P("section", "grp", "tp"),
        P(),
        P("grp", ("section", "tp")),
        P("grp", ("section", "tp")),
        P(("section", "tp")),
        P(("section", "tp")),
    )
    return jax.shard_map(
        local,
        mesh=mesh,
        in_specs=placed,
        out_specs=(
            P("section", "grp", "tp"),
            P(None, "grp", ("section", "tp")),
            P(None, "grp", ("section", "tp")),
        ),
        check_vma=False,
    )
```
